32 devices in a mesh: row: 8 (over z, core), col: 4 (over y, x).
Axes of the slice: x: 2, y: 2, z: 4, core: 2. Of those that a mesh axis runs over, the one named last changes fastest.
Arguments:
- act_codes: int32 [512, 7168], P('col', 'row'), may hold values from -127 to 127
- act_scales: float32 [512, 112], P('col', 'row'), may hold values from 0.005 to 0.03
- gate_weight: bfloat16 [7168, 18432], P('row', 'col'), may hold values from -0.0625 to 0.0625
- up_weight: bfloat16 [7168, 18432], P('row', 'col'), may hold values from -0.0625 to 0.0625
- down_weight: bfloat16 [18432, 7168], P('col', 'row'), may hold values from -0.046875 to 0.046875
Outputs:
- mixed: bfloat16 [512, 7168], P('col', 'row')
The draws below stay inside these ranges and needn't reach their ends.
All inputs are finite; a program needn't handle non-finite values.
Results may differ from the reference program's by a relative error of at most 0.03.
Values may be sent and summed in bfloat16 or wider, within the bound.
A program may use at most 128 MiB of HBM per device.

```python
import math
import jax
import jax.numpy as jnp
from jax import lax

D = 7168
FF = 18432
QB = 64
TOKENS = 512
D_ROW = 896
FF_COL = 4608
BLOCKS = 112
N_ROW = 8
N_COL = 4


def place_ends(entries, rng, least, top_value):
    index_at = [jax.random.randint(jax.random.fold_in(rng, axis), (), 0, length) for axis, length in enumerate(entries.shape)]
    widest = entries.shape.index(max(entries.shape))
    next_to = index_at[:widest] + [(index_at[widest] + 1) % entries.shape[widest]] + index_at[widest + 1:]
    return entries.at[tuple(index_at)].set(least).at[tuple(next_to)].set(top_value)


def shard_levels(own_key, dims, cuts, smallest, high):
    loudness, own = 1.0, jax.random.fold_in(own_key, 6)
    for axis_at, blocks in cuts:
        steps = jnp.exp(jax.random.uniform(jax.random.fold_in(own, axis_at), (blocks,), jnp.float32, smallest / len(cuts), high / len(cuts)))
        loudness = loudness * jnp.repeat(steps, dims[axis_at] // blocks).reshape([-1 if axis == axis_at else 1 for axis in range(len(dims))])
    return loudness


def centred(key, extent, width, most, cuts=(), kind=jnp.bfloat16):
    values = jax.random.normal(key, extent, jnp.float32) * width
    if len(cuts) > 0:
        values = shard_levels(key, extent, cuts, -0.22, 0.18) * values
    return jnp.clip(values, min=-most, max=most).astype(kind)


def setup_inputs(seed: int = 0) -> dict:
    keys = jax.random.split(jax.random.key(seed), 6)
    act_codes = place_ends(jax.random.randint(keys[0], (TOKENS, D), -127, 128), jax.random.fold_in(keys[0], 1), -127, 127).astype(jnp.int32)
    act_scales = jnp.clip(jnp.exp(math.log(0.03) - 1.7917595 * jax.random.uniform(keys[1], (TOKENS, BLOCKS), jnp.float32) ** shard_levels(keys[1], (TOKENS, BLOCKS), ((0, 4), (1, 8)), -0.2, 0.2)), 0.005, 0.03)
    gate_weight = centred(keys[2], (D, FF), D ** -0.5, 0.0625, ((0, 8), (1, 4)))
    up_weight = centred(keys[3], (D, FF), D ** -0.5, 0.0625, ((0, 8), (1, 4)))
    down_weight = centred(keys[4], (FF, D), FF ** -0.5, 0.046875, ((0, 4), (1, 8)))
    return dict(act_codes=act_codes, act_scales=act_scales, gate_weight=gate_weight, up_weight=up_weight, down_weight=down_weight)


def dequantize(act_codes, act_scales):
    rows = act_codes.shape[0]
    blocked = act_codes.astype(jnp.float32).reshape(rows, BLOCKS, QB)
    scaled = blocked * act_scales[:, :, None]
    return scaled.reshape(rows, D).astype(jnp.bfloat16)


def rounded(value):
    narrow = lax.optimization_barrier(value.astype(jnp.bfloat16))
    return narrow.astype(jnp.float32)


def reference(act_codes, act_scales, gate_weight, up_weight, down_weight):
    acts = dequantize(act_codes, act_scales)

    def feature_group(index, totals):
        start = (index * D_ROW).astype(jnp.int32)
        slab = lax.dynamic_slice_in_dim(acts, start, D_ROW, 1)
        gate_rows = lax.dynamic_slice_in_dim(gate_weight, start, D_ROW, 0)
        up_rows = lax.dynamic_slice_in_dim(up_weight, start, D_ROW, 0)
        gate_part = rounded(jnp.dot(slab, gate_rows, preferred_element_type=jnp.float32))
        up_part = rounded(jnp.dot(slab, up_rows, preferred_element_type=jnp.float32))
        return (totals[0] + gate_part, totals[1] + up_part)

    empty = jnp.zeros((TOKENS, FF), jnp.float32)
    gate, up = lax.fori_loop(0, N_ROW, feature_group, (empty, empty))
    hidden = (jax.nn.silu(gate) * up).astype(jnp.bfloat16)

    def hidden_group(index, total):
        start = (index * FF_COL).astype(jnp.int32)
        slab = lax.dynamic_slice_in_dim(hidden, start, FF_COL, 1)
        rows_down = lax.dynamic_slice_in_dim(down_weight, start, FF_COL, 0)
        return total + rounded(jnp.dot(slab, rows_down, preferred_element_type=jnp.float32))

    mixed = lax.fori_loop(0, N_COL, hidden_group, jnp.zeros((TOKENS, D), jnp.float32))
    return mixed.astype(jnp.bfloat16)
```

```python
import functools

import jax
import jax.numpy as jnp
from jax import lax
from jax.experimental import pallas as pl
from jax.experimental.pallas import tpu as pltpu
from jax.sharding import PartitionSpec as P

MESH = pl.DeviceIdType.MESH
GROUPS = 2
WIDTHS = (256, 384, 128)
AHEAD = 2
ROWS_PER_DOT = 256
HOP_STEPS = 2


def body(
    n_row, n_col, x_ref, gate_hbm, up_hbm, down_hbm, o_ref,
    every, gate_w, up_w, down_w, part, from_core, from_chip, hid, acc, out_send, out_recv,
    w_sem, act_s, act_r, core_s, core_r, chip_s, chip_r, hz_s, hz_r, hc_s, hc_r, out_s, out_r,
):
    groups, _, piece, depth = x_ref.shape
    chunks, _, width = gate_w.shape
    steps = groups * chunks
    n_chip = n_row // 2
    rows = n_col * piece

    row, col = lax.axis_index("row"), lax.axis_index("col")
    chip, core = row // 2, row % 2
    pos = jnp.where(core == 0, chip, n_chip - 1 - chip)
    ahead_row = row + jnp.where(core == 0, 2, -2)
    behind_row = row - jnp.where(core == 0, 2, -2)
    other_row = chip * 2 + 1 - core
    is_first, is_last = pos == 0, pos == n_chip - 1

    def weight_copy(kind, j):
        columns = pl.ds(j * width, width)
        if kind == 0:
            return pltpu.make_async_copy(gate_hbm.at[:, columns], gate_w.at[j], w_sem.at[0, j])
        if kind == 1:
            return pltpu.make_async_copy(up_hbm.at[:, columns], up_w.at[j], w_sem.at[1, j])
        return pltpu.make_async_copy(down_hbm.at[columns, :], down_w.at[j], w_sem.at[2, j])

    for j in range(chunks):
        weight_copy(0, j).start()
        weight_copy(1, j).start()

    barrier = pltpu.get_barrier_semaphore()
    for p in range(1, n_col):
        pl.semaphore_signal(barrier, inc=1, device_id={"col": lax.rem(col + p, n_col)}, device_id_type=MESH)
    pl.semaphore_signal(barrier, inc=1, device_id={"row": other_row}, device_id_type=MESH)

    @pl.when(chip > 0)
    def _():
        pl.semaphore_signal(barrier, inc=1, device_id={"row": row - 2}, device_id_type=MESH)

    @pl.when(chip < n_chip - 1)
    def _():
        pl.semaphore_signal(barrier, inc=1, device_id={"row": row + 2}, device_id_type=MESH)

    neighbours = jnp.where(chip > 0, 1, 0) + jnp.where(chip < n_chip - 1, 1, 0)
    pl.semaphore_wait(barrier, n_col + neighbours)

    def remote(src, dst, send, recv, where):
        return pltpu.make_async_remote_copy(
            src_ref=src, dst_ref=dst, send_sem=send, recv_sem=recv, device_id=where, device_id_type=MESH
        )

    def act_copy(g, p):
        return remote(
            x_ref.at[g], every.at[g, :, col], act_s.at[g, p], act_r.at[g, col], {"col": lax.rem(col + p, n_col)}
        )

    def act_arrival(g, p):
        source = lax.rem(col + p, n_col)
        return remote(x_ref.at[g], every.at[g, :, source], act_s.at[g, p], act_r.at[g, source], {"col": source})

    def core_copy(j):
        return remote(part.at[j, 1 - core], from_core.at[j], core_s.at[j], core_r.at[j], {"row": other_row})

    def chip_copy(j):
        return remote(part.at[j, core], from_chip.at[j], chip_s.at[j], chip_r.at[j], {"row": ahead_row})

    def hidden_back(j):
        return remote(hid.at[j, core], hid.at[j, core], hz_s.at[j], hz_r.at[j], {"row": behind_row})

    def hidden_across(j):
        return remote(hid.at[j, core], hid.at[j, core], hc_s.at[j], hc_r.at[j], {"row": other_row})

    def hidden_crossed(j):
        return remote(hid.at[j, 1 - core], hid.at[j, 1 - core], hc_s.at[j], hc_r.at[j], {"row": other_row})

    def out_copy(g, p):
        peer = lax.rem(col + p, n_col)
        return remote(out_send.at[g, peer], out_recv.at[g, col], out_s.at[g, p], out_r.at[g, col], {"col": peer})

    def out_arrival(g, p):
        source = lax.rem(col + p, n_col)
        return remote(out_send.at[g, source], out_recv.at[g, source], out_s.at[g, p], out_r.at[g, source], {"col": source})

    for g in range(groups):
        for p in range(1, n_col):
            act_copy(g, p).start()
        for side in range(2):
            every[g, side, col] = x_ref[g, side]
    for j in range(chunks):
        weight_copy(2, j).start()
    acc[...] = jnp.zeros_like(acc)

    tile = min(ROWS_PER_DOT, 2 * rows)
    side_tile = min(tile, rows)

    def multiply(j):
        g, jj = j // chunks, lax.rem(j, chunks)

        @pl.when(jj == 0)
        def _():
            for p in range(1, n_col):
                act_arrival(g, p).wait_recv()

        @pl.when(g == 0)
        def _():
            weight_copy(0, jj).wait()
            weight_copy(1, jj).wait()

        taken = tile // piece
        for side_at in range(0, 2 * n_col, taken):
            if taken > n_col:
                x = every[g].reshape(2 * rows, depth)
            else:
                x = every[g, side_at // n_col, side_at % n_col:side_at % n_col + taken].reshape(tile, depth)
            for half, w in enumerate((gate_w, up_w)):
                y = jnp.dot(x, w[jj], preferred_element_type=jnp.float32).astype(jnp.bfloat16)
                lanes = slice(half * width, (half + 1) * width)
                if taken > n_col:
                    part[j, :, :, lanes] = y.reshape(2, rows, width)
                else:
                    first = (side_at % n_col) * piece
                    part[j, side_at // n_col, first:first + tile, lanes] = y
        core_copy(j).start()

    def add_up(j):
        core_copy(j).wait_recv()

        @pl.when(is_first)
        def _():
            for r in range(0, rows, side_tile):
                at = slice(r, r + side_tile)
                part[j, core, at] = (
                    part[j, core, at].astype(jnp.float32) + from_core[j, at].astype(jnp.float32)
                ).astype(jnp.bfloat16)
            chip_copy(j).start()

        @pl.when(jnp.logical_not(is_first))
        def _():
            chip_copy(j).wait_recv()

        @pl.when(jnp.logical_not(is_first) & jnp.logical_not(is_last))
        def _():
            for r in range(0, rows, side_tile):
                at = slice(r, r + side_tile)
                part[j, core, at] = (
                    part[j, core, at].astype(jnp.float32)
                    + from_core[j, at].astype(jnp.float32)
                    + from_chip[j, at].astype(jnp.float32)
                ).astype(jnp.bfloat16)
            chip_copy(j).start()

        @pl.when(is_last)
        def _():
            for r in range(0, rows, side_tile):
                at = slice(r, r + side_tile)

                def total(lanes):
                    return (
                        part[j, core, at, lanes].astype(jnp.float32)
                        + from_core[j, at, lanes].astype(jnp.float32)
                        + from_chip[j, at, lanes].astype(jnp.float32)
                    )

                gate, up = total(slice(0, width)), total(slice(width, 2 * width))
                hid[j, core, at] = (gate / (1.0 + jnp.exp(-gate)) * up).astype(jnp.bfloat16)
            hidden_back(j).start()
            hidden_across(j).start()

    def pass_on(j):
        hidden_back(j).wait_recv()

        @pl.when(jnp.logical_not(is_first))
        def _():
            hidden_back(j).start()

        hidden_across(j).start()

    def multiply_down(j):
        jj = lax.rem(j, chunks)
        hidden_crossed(j).wait_recv()

        @pl.when(j < chunks)
        def _():
            weight_copy(2, jj).wait()

        for r in range(0, 2 * rows, tile):
            if tile > rows:
                h = hid[j].reshape(2 * rows, width)
            else:
                h = hid[j, r // rows, r % rows:r % rows + tile]
            acc[r:r + tile] += jnp.dot(h, down_w[jj], preferred_element_type=jnp.float32)

    def hand_out(g):
        for side in range(2):
            for k in range(n_col):
                first = side * rows + k * piece
                out_send[g, k, side] = acc[first:first + piece].astype(jnp.bfloat16)
        acc[...] = jnp.zeros_like(acc)
        for p in range(1, n_col):
            out_copy(g, p).start()

    lag = jnp.maximum(HOP_STEPS * 2 * (n_chip - 1 - pos), 1)
    down_lag = jnp.maximum(lag, HOP_STEPS * (n_chip - 1) + 1)

    early = AHEAD + HOP_STEPS * jnp.maximum(2 * pos - (n_chip - 1), 0)
    early = jnp.minimum(early, steps)

    def begin(j, carry):
        multiply(j)
        return carry

    lax.fori_loop(0, early, begin, 0)

    def step(i, carry):
        @pl.when(i + early < steps)
        def _():
            multiply(i + early)

        @pl.when(i < steps)
        def _():
            add_up(i)

        @pl.when((i >= lag) & (i - lag < steps) & jnp.logical_not(is_last))
        def _():
            pass_on(i - lag)

        @pl.when(i >= down_lag)
        def _():
            j = i - down_lag
            multiply_down(j)

            @pl.when(lax.rem(j, chunks) == chunks - 1)
            def _():
                hand_out(j // chunks)

        return carry

    lax.fori_loop(0, steps + down_lag, step, 0)

    for g in range(groups):
        for p in range(1, n_col):
            out_arrival(g, p).wait_recv()
        for side in range(2):
            total = out_send[g, col, side].astype(jnp.float32)
            for p in range(1, n_col):
                total += out_recv[g, lax.rem(col + p, n_col), side].astype(jnp.float32)
            o_ref[g, side] = total.astype(o_ref.dtype)

    def drain(j, carry):
        core_copy(j).wait_send()
        hidden_across(j).wait_send()

        @pl.when(jnp.logical_not(is_last))
        def _():
            chip_copy(j).wait_send()

        @pl.when(jnp.logical_not(is_first))
        def _():
            hidden_back(j).wait_send()

        return carry

    lax.fori_loop(0, steps, drain, 0)
    for g in range(groups):
        for p in range(1, n_col):
            act_copy(g, p).wait_send()
            out_copy(g, p).wait_send()


def on_device(n_row, n_col, act_codes, act_scales, gate_weight, up_weight, down_weight):
    tokens, depth = act_codes.shape
    nblocks = act_scales.shape[1]
    hidden, out_width = down_weight.shape
    blocked = act_codes.astype(jnp.float32).reshape(tokens, nblocks, depth // nblocks)
    acts = (blocked * act_scales[:, :, None]).reshape(tokens, depth).astype(jnp.bfloat16)

    groups = GROUPS
    piece = tokens // (2 * groups)
    width = next(w for w in WIDTHS if hidden % w == 0)
    chunks = hidden // width
    steps = groups * chunks
    rows = n_col * piece
    bf16 = jnp.bfloat16
    dma = pltpu.SemaphoreType.DMA
    out = pl.pallas_call(
        functools.partial(body, n_row, n_col),
        out_shape=jax.ShapeDtypeStruct((groups, 2, piece, out_width), bf16),
        in_specs=[pl.BlockSpec(memory_space=pltpu.VMEM)] + [pl.BlockSpec(memory_space=pl.ANY)] * 3,
        out_specs=pl.BlockSpec(memory_space=pltpu.VMEM),
        scratch_shapes=[
            pltpu.VMEM((groups, 2, n_col, piece, depth), bf16),
            pltpu.VMEM((chunks, depth, width), bf16),
            pltpu.VMEM((chunks, depth, width), bf16),
            pltpu.VMEM((chunks, width, out_width), bf16),
            pltpu.VMEM((steps, 2, rows, 2 * width), bf16),
            pltpu.VMEM((steps, rows, 2 * width), bf16),
            pltpu.VMEM((steps, rows, 2 * width), bf16),
            pltpu.VMEM((steps, 2, rows, width), bf16),
            pltpu.VMEM((2 * rows, out_width), jnp.float32),
            pltpu.VMEM((groups, n_col, 2, piece, out_width), bf16),
            pltpu.VMEM((groups, n_col, 2, piece, out_width), bf16),
            dma((3, chunks)),
            dma((groups, n_col)),
            dma((groups, n_col)),
        ]
        + [dma((steps,))] * 8
        + [dma((groups, n_col))] * 2,
        compiler_params=pltpu.CompilerParams(
            collective_id=0, has_side_effects=True, vmem_limit_bytes=67043328
        ),
    )(acts.reshape(groups, 2, piece, depth), gate_weight, up_weight, down_weight)
    return out.reshape(tokens, out_width)


def solution(mesh):
    placed = (P("col", "row"), P("col", "row"), P("row", "col"), P("row", "col"), P("col", "row"))
    return jax.shard_map(
        functools.partial(on_device, mesh.shape["row"], mesh.shape["col"]),
        mesh=mesh,
        in_specs=placed,
        out_specs=P("col", "row"),
        check_vma=False,
    )
```
